512 devices in a mesh: blk: 512 (over x, z, y, core).
Axes of the slice: x: 4, y: 4, z: 16, core: 2. Of those that a mesh axis runs over, the one named last changes fastest.
Arguments:
- x_points: bfloat16 [16384, 128], P('blk'), may hold values from -5.2 to 5.2, as said below
- y_points: bfloat16 [16384, 128], P('blk'), may hold values from -5.2 to 5.2, as said below
Outputs:
- x_scores: float32 [16384, 3], P('blk')
- y_scores: float32 [16384, 3], P('blk')
- mmd_stat: float32 [3], replicated
- hsic_stat: float32 [3], replicated
The draws below stay inside these ranges and needn't reach their ends.
Inputs may be any that keep to these rules, and one draw needn't show every extreme that they name: `x_points`: every entry of the first sample lies within -5.2 and 5.2. `y_points`: every entry of the second sample lies within -5.2 and 5.2.
All inputs are finite; a program needn't handle non-finite values.
Results may differ from the reference program's by a relative error of at most 0.00035.
Values may be sent and summed in bfloat16 or wider, within the bound.
A program may use at most 64 MiB of HBM per device.

```python
import jax
import jax.numpy as jnp
from jax import lax

D = 128
PTS_DEV = 32
POINTS = 16384
N_BLK = 512


def clustered(key, member):
    labels = jax.random.randint(jax.random.fold_in(key, 7), (POINTS,), 0, POINTS // 4)
    centres = jnp.clip(jax.random.normal(jax.random.fold_in(key, 20 + member), (POINTS // 4, D), jnp.float32), -4.0, 4.0)
    noise_key = jax.random.fold_in(key, 40 + member)
    spread = jnp.clip(jax.random.normal(noise_key, (POINTS, D), jnp.float32), -4.0, 4.0)
    return (centres[labels] + 0.3 * spread).astype(jnp.bfloat16)


def draw_x_points(key, part):
    return clustered(key, 0)


def draw_y_points(key, part):
    return clustered(key, 1)


def setup_inputs(seed: int = 0) -> dict:
    keys = jax.random.split(jax.random.key(seed), 3)
    return {
        "x_points": draw_x_points(jax.random.fold_in(keys[2], 71), 0),
        "y_points": draw_y_points(jax.random.fold_in(keys[2], 71), 0),
    }


WIDTHS = (0.08, 0.16, 0.32)


def kernels(left, right):
    products = jnp.dot(left, right.T, preferred_element_type=jnp.float32)
    left_sq = jnp.sum(jnp.square(left.astype(jnp.float32)), axis=1)
    right_sq = jnp.sum(jnp.square(right.astype(jnp.float32)), axis=1)
    distance = jnp.maximum(left_sq[:, None] + right_sq[None, :] - 2.0 * products, 0.0)
    factor = 1.0 / (2.0 * jnp.array(WIDTHS, jnp.float32) * left.shape[1])
    return jnp.exp(-factor[:, None, None] * distance[None])


def reference(x_points, y_points):
    def block_rows(offset):
        left_x = lax.dynamic_slice_in_dim(x_points, offset, PTS_DEV, 0)
        left_y = lax.dynamic_slice_in_dim(y_points, offset, PTS_DEV, 0)
        row_index = offset + jnp.arange(PTS_DEV, dtype=jnp.int32)
        col_index = jnp.arange(POINTS, dtype=jnp.int32)
        offdiag = (row_index[:, None] != col_index[None, :]).astype(jnp.float32)
        raw_x = kernels(left_x, x_points)
        raw_y = kernels(left_y, y_points)
        cross_xy = kernels(left_x, y_points)
        cross_yx = kernels(left_y, x_points)
        hadamard = raw_x * raw_y
        return jnp.stack([jnp.sum(raw_x * offdiag, 2), jnp.sum(raw_y * offdiag, 2), jnp.sum(cross_xy, 2), jnp.sum(cross_yx, 2), jnp.sum(hadamard, 2)])

    offsets = jnp.arange(N_BLK, dtype=jnp.int32) * PTS_DEV
    blocks = lax.map(block_rows, offsets)
    sums = jnp.transpose(blocks, (1, 2, 0, 3)).reshape(5, 3, POINTS)
    sum_xx, sum_yy, sum_xy, sum_yx, sum_h = sums[0], sums[1], sums[2], sums[3], sums[4]
    full_x = sum_xx + 1.0
    full_y = sum_yy + 1.0
    count_all = jnp.float32(POINTS)
    mmd_stat = count_all * ((jnp.sum(sum_xx, 1) + jnp.sum(sum_yy, 1)) / (count_all * (count_all - 1.0)) - 2.0 * jnp.sum(sum_xy, 1) / (count_all * count_all))
    hsic_stat = (jnp.sum(sum_h, 1) - 2.0 * jnp.sum(full_x * full_y, 1) / count_all + jnp.sum(full_x, 1) * jnp.sum(full_y, 1) / (count_all * count_all)) / count_all
    x_scores = (jnp.log(sum_xx) - jnp.log(sum_xy)).T
    y_scores = (jnp.log(sum_yy) - jnp.log(sum_yx)).T
    return x_scores, y_scores, mmd_stat, hsic_stat
```

```python
import functools
import math

import jax
import jax.numpy as jnp
from jax import lax
from jax.experimental import pallas as pl
from jax.experimental.pallas import tpu as pltpu
from jax.sharding import PartitionSpec as P

MESH = pl.DeviceIdType.MESH
NX, NZ, NY, NC = 4, 16, 4, 2
PLANE = NX * NY * NC
PTS = 32
DIM = 128
TILES = PLANE * PTS // 128
SCALE = math.log2(math.e) / (2.0 * 0.32 * DIM)
NT = (((1,), (1,)), ((), ()))
F32 = jnp.float32
BF16 = jnp.bfloat16


def device_of(x, z, y, c):
    return ((x * NZ + z) * NY + y) * NC + c


def plane_device(q, z):
    return device_of(q // (NY * NC), z, (q // NC) % NY, q % NC)


def squares(points):
    wide = points.astype(F32)
    sq = wide * wide
    high = sq.astype(BF16)
    low = (sq - high.astype(F32)).astype(BF16)
    return high, low


def fold(tile):
    return jnp.sum(tile.reshape(-1, 8, 128), axis=0)


def powers(e):
    e2 = e * e
    return e2 * e2, e2, e


def kernel(x_hbm, y_hbm, xs_ref, ys_ref, mmd_ref, hsic_ref,
           zbuf, pbuf, rown, acc, sbuf, rbuf, tsend, trecv, usend, urecv,
           load_sem, zsend_sem, zrecv_sem, psend_sem, precv_sem, ssend_sem, srecv_sem,
           tsend_sem, trecv_sem, usend_sem, urecv_sem):
    me = lax.axis_index("blk")
    c = me % NC
    y = (me // NC) % NY
    z = (me // (NC * NY)) % NZ
    x = me // (NC * NY * NZ)
    q = (x * NY + y) * NC + c

    loads = []
    for n, (buf, slot) in enumerate(((zbuf, z), (pbuf, q))):
        for k, src in enumerate((x_hbm, y_hbm)):
            cp = pltpu.make_async_copy(src, buf.at[slot, pl.ds(PTS * k, PTS)], load_sem.at[2 * n + k])
            cp.start()
            loads.append(cp)

    barrier = pltpu.get_barrier_semaphore()

    def greet_z(d, carry):
        pl.semaphore_signal(barrier, inc=1, device_id=(device_of(x, (z + d) % NZ, y, c),), device_id_type=MESH)
        return carry

    def greet_p(d, carry):
        pl.semaphore_signal(barrier, inc=1, device_id=(plane_device((q + d) % PLANE, z),), device_id_type=MESH)
        return carry

    lax.fori_loop(1, NZ, greet_z, 0)
    lax.fori_loop(1, PLANE, greet_p, 0)
    for cp in loads:
        cp.wait()
    pl.semaphore_wait(barrier, NZ + PLANE - 2)

    def offset(d):
        return jnp.where(d % 2 == 1, (d + 1) // 2, NZ - d // 2)

    def send_z(d, carry):
        to = (z + offset(d)) % NZ
        pltpu.make_async_remote_copy(
            src_ref=zbuf.at[z], dst_ref=zbuf.at[z], send_sem=zsend_sem, recv_sem=zrecv_sem.at[z],
            device_id=(device_of(x, to, y, c),), device_id_type=MESH).start()
        return carry

    def send_p(d, carry):
        pltpu.make_async_remote_copy(
            src_ref=zbuf.at[z], dst_ref=pbuf.at[q], send_sem=psend_sem, recv_sem=precv_sem,
            device_id=(plane_device((q + d) % PLANE, z),), device_id_type=MESH).start()
        return carry

    lax.fori_loop(0, NZ - 1, lambda i, carry: send_z(NZ - 1 - i, carry), 0)
    lax.fori_loop(1, PLANE, send_p, 0)

    def wait_bytes(ref, sem):
        pltpu.make_async_copy(ref, ref, sem).wait()

    wait_bytes(pbuf.at[pl.ds(0, PLANE - 1)], precv_sem)

    acc[...] = jnp.zeros_like(acc)
    ones8 = jnp.ones((8, DIM), BF16)
    for g in range(TILES):
        for k in range(2):
            pts = pbuf[4 * g:4 * g + 4, PTS * k:PTS * k + PTS, :].reshape(128, DIM)
            high, low = squares(pts)
            norm = lax.dot_general(ones8, high, NT, preferred_element_type=F32)
            norm += lax.dot_general(ones8, low, NT, preferred_element_type=F32)
            rown[g, k] = norm * -SCALE

    def block(zi, diagonal):
        cols = zbuf[zi]
        high, low = squares(cols)
        ones = jnp.ones((DIM, 128), BF16)
        coln = jnp.dot(high, ones, preferred_element_type=F32) + jnp.dot(low, ones, preferred_element_type=F32)
        coln = coln * -SCALE
        for g in range(TILES):
            rows_x = pbuf[4 * g:4 * g + 4, 0:PTS, :].reshape(128, DIM)
            rows_y = pbuf[4 * g:4 * g + 4, PTS:2 * PTS, :].reshape(128, DIM)
            prod_x = lax.dot_general(cols, rows_x, NT, preferred_element_type=F32)
            prod_y = lax.dot_general(cols, rows_y, NT, preferred_element_type=F32)

            def gauss(prod, k, row):
                arg = prod * (2.0 * SCALE) + coln[PTS * k:PTS * k + PTS]
                arg = (arg.reshape(-1, 8, 128) + rown[g, row][None]).reshape(PTS, 128)
                return powers(jnp.exp2(jnp.minimum(arg, 0.0)))

            xx = gauss(prod_x[:PTS], 0, 0)
            xy = gauss(prod_x[PTS:], 1, 0)
            yx = gauss(prod_y[:PTS], 0, 1)
            yy = gauss(prod_y[PTS:], 1, 1)
            hh = [a * b for a, b in zip(xx, yy)]
            if diagonal:
                lane = lax.broadcasted_iota(jnp.int32, (PTS, 128), 1) + 128 * g
                sub = lax.broadcasted_iota(jnp.int32, (PTS, 128), 0) + PTS * q
                off = lane != sub
                xx = [jnp.where(off, a, 0.0) for a in xx]
                yy = [jnp.where(off, a, 0.0) for a in yy]
            for t, stat in enumerate((xx, yy, xy, yx, hh)):
                for b in range(3):
                    acc[g, t * 3 + b] += fold(stat[b])

    block(z, True)

    def step(d, carry):
        zi = (z + offset(d)) % NZ
        pltpu.make_async_copy(zbuf.at[zi], zbuf.at[zi], zrecv_sem.at[zi]).wait()
        block(zi, False)
        return carry

    lax.fori_loop(1, NZ, step, 0)

    for g in range(TILES):
        def row(t, b):
            return jnp.sum(acc[g, t * 3 + b], axis=0, keepdims=True)
        zero = jnp.zeros((1, 128), F32)
        groups = [jnp.concatenate([row(k, 0), row(k, 1), row(k, 2), row(4, k) if k < 3 else zero], axis=0) for k in range(4)]
        for m in range(4):
            sbuf[4 * g + m] = jnp.concatenate([groups[k][:, PTS * m:PTS * m + PTS] for k in range(4)], axis=1)

    def send_s(d, carry):
        to = (q + d) % PLANE
        pltpu.make_async_remote_copy(
            src_ref=sbuf.at[to], dst_ref=rbuf.at[q], send_sem=ssend_sem, recv_sem=srecv_sem,
            device_id=(plane_device(to, z),), device_id_type=MESH).start()
        return carry

    lax.fori_loop(1, PLANE, send_s, 0)
    rbuf[q] = sbuf[q]
    wait_bytes(rbuf.at[pl.ds(0, PLANE - 1)], srecv_sem)
    sums = jnp.sum(rbuf[...], axis=0)
    full = sums + 1.0
    prod = full * pltpu.roll(full, 128 - PTS, 1)
    lane = lax.broadcasted_iota(jnp.int32, (4, 128), 1)
    sub = lax.broadcasted_iota(jnp.int32, (4, 128), 0)
    packed = jnp.zeros((4, 128), F32)
    for k in range(5):
        src = prod if k == 4 else sums
        lo = PTS * (k % 4)
        tot = jnp.sum(jnp.where((lane >= lo) & (lane < lo + PTS), src, 0.0), axis=1, keepdims=True)
        packed = jnp.where(lane == 8 * sub + k, tot, packed)
    tsend[...] = jnp.sum(packed, axis=0, keepdims=True)

    def send_t(d, carry):
        pltpu.make_async_remote_copy(
            src_ref=tsend, dst_ref=trecv.at[q], send_sem=tsend_sem, recv_sem=trecv_sem,
            device_id=(plane_device((q + d) % PLANE, z),), device_id_type=MESH).start()
        return carry

    lax.fori_loop(1, PLANE, send_t, 0)
    trecv[q] = tsend[...]

    logs = jnp.log(sums)
    score = logs - pltpu.roll(logs, 64, 1)
    score = jnp.concatenate([score, score], axis=0)
    turned = jnp.transpose(jnp.concatenate([score] * 16, axis=0))
    xs_ref[...] = turned[0:PTS, 0:3]
    ys_ref[...] = turned[PTS:2 * PTS, 0:3]

    wait_bytes(trecv.at[pl.ds(0, PLANE - 1)], trecv_sem)
    usend[...] = jnp.sum(trecv[...], axis=0)

    def send_u(d, carry):
        pltpu.make_async_remote_copy(
            src_ref=usend, dst_ref=urecv.at[z], send_sem=usend_sem, recv_sem=urecv_sem,
            device_id=(device_of(x, (z + d) % NZ, y, c),), device_id_type=MESH).start()
        return carry

    lax.fori_loop(1, NZ, send_u, 0)
    urecv[z] = usend[...]
    wait_bytes(urecv.at[pl.ds(0, NZ - 1)], urecv_sem)
    tot = jnp.broadcast_to(jnp.sum(urecv[...], axis=0), (8, 128))

    n = float(PTS * PLANE * NZ)

    def at(k, b):
        return tot[0:1, 8 * b + k:8 * b + k + 1]

    for b in range(3):
        txx, tyy, txy, tpr = at(0, b), at(1, b), at(2, b), at(4, b)
        th = tot[0:1, 8 * 3 + b:8 * 3 + b + 1]
        mmd_ref[0:1, b:b + 1] = n * ((txx + tyy) / (n * (n - 1.0)) - 2.0 * txy / (n * n))
        hsic_ref[0:1, b:b + 1] = (th - 2.0 * tpr / n + (txx + n) * (tyy + n) / (n * n)) / n

    wait_bytes(zbuf.at[pl.ds(0, NZ - 1)], zsend_sem)
    wait_bytes(pbuf.at[pl.ds(0, PLANE - 1)], psend_sem)
    wait_bytes(sbuf.at[pl.ds(0, PLANE - 1)], ssend_sem)
    wait_bytes(trecv.at[pl.ds(0, PLANE - 1)], tsend_sem)
    wait_bytes(urecv.at[pl.ds(0, NZ - 1)], usend_sem)


def shards(x_points, y_points):
    dma = pltpu.SemaphoreType.DMA
    vmem = pl.BlockSpec(memory_space=pltpu.VMEM)
    xs, ys, mmd, hsic = pl.pallas_call(
        kernel,
        out_shape=(
            jax.ShapeDtypeStruct((PTS, 3), F32),
            jax.ShapeDtypeStruct((PTS, 3), F32),
            jax.ShapeDtypeStruct((1, 3), F32),
            jax.ShapeDtypeStruct((1, 3), F32),
        ),
        in_specs=[pl.BlockSpec(memory_space=pl.ANY)] * 2,
        out_specs=(vmem,) * 4,
        scratch_shapes=[
            pltpu.VMEM((NZ, 2 * PTS, DIM), BF16),
            pltpu.VMEM((PLANE, 2 * PTS, DIM), BF16),
            pltpu.VMEM((TILES, 2, 8, 128), F32),
            pltpu.VMEM((TILES, 15, 8, 128), F32),
            pltpu.VMEM((PLANE, 4, 128), F32),
            pltpu.VMEM((PLANE, 4, 128), F32),
            pltpu.VMEM((1, 128), F32),
            pltpu.VMEM((PLANE, 1, 128), F32),
            pltpu.VMEM((1, 128), F32),
            pltpu.VMEM((NZ, 1, 128), F32),
            dma((4,)), dma, dma((NZ,)), dma, dma, dma, dma, dma, dma, dma, dma,
        ],
        compiler_params=pltpu.CompilerParams(collective_id=0, has_side_effects=True),
        name="mmd_hsic",
    )(x_points, y_points)
    return xs, ys, mmd.reshape(3), hsic.reshape(3)


def solution(mesh):
    return jax.shard_map(
        shards,
        mesh=mesh,
        in_specs=(P("blk", None), P("blk", None)),
        out_specs=(P("blk", None), P("blk", None), P(), P()),
        check_vma=False,
    )
```

```python
import functools
import math

import jax
import jax.numpy as jnp
from jax import lax
from jax.experimental import pallas as pl
from jax.experimental.pallas import tpu as pltpu
from jax.sharding import PartitionSpec as P

MESH = pl.DeviceIdType.MESH
NX, NZ, NY, NC = 4, 16, 4, 2
PLANE = NX * NY * NC
PTS = 32
STRIDE = 4
DIM = 128
TILES = PLANE * PTS // 128
SCALE = math.log2(math.e) / (2.0 * 0.32 * DIM)
NT = (((1,), (1,)), ((), ()))
F32 = jnp.float32
BF16 = jnp.bfloat16


def device_of(x, z, y, c):
    return ((x * NZ + z) * NY + y) * NC + c


def squares(points):
    wide = points.astype(F32)
    sq = wide * wide
    high = sq.astype(BF16)
    low = (sq - high.astype(F32)).astype(BF16)
    return high, low


def fold(tile):
    return jnp.sum(tile.reshape(-1, 8, 128), axis=0)


def powers(e):
    e2 = e * e
    return e2 * e2, e2, e


def kernel(x_hbm, y_hbm, xs_ref, ys_ref, mmd_ref, hsic_ref,
           zbuf, pbuf, rown, coln, acc, sbuf, rbuf, tsend, trecv, usend, urecv,
           load_sem, zsend_sem, zrecv_sem, psend_sem, precv_sem, dsend_sem, drecv_sem, ssend_sem, srecv_sem,
           tsend_sem, trecv_sem, usend_sem, urecv_sem):
    me = lax.axis_index("blk")
    c = lax.rem(me, NC)
    y = lax.rem(me // NC, NY)
    z = lax.rem(me // (NC * NY), NZ)
    x = me // (NC * NY * NZ)
    chip = x * NY + y
    q = c * (NX * NY) + chip

    loads = []
    for n, buf in enumerate((zbuf.at[0], pbuf.at[q])):
        for k, src in enumerate((x_hbm, y_hbm)):
            cp = pltpu.make_async_copy(src, buf.at[pl.ds(PTS * k, PTS)], load_sem.at[2 * n + k])
            cp.start()
            loads.append(cp)

    def z_peer(off):
        return (device_of(x, lax.rem(z + (off + NZ), NZ), y, c),)

    def plane_peer(dx, dy, dc):
        px, py, pc = lax.rem(x + dx, NX), lax.rem(y + dy, NY), lax.rem(c + dc, NC)
        return (device_of(px, z, py, pc),), pc * (NX * NY) + px * NY + py

    def far(v):
        return min(v, 4 - v)

    moves = sorted(((dx, dy) for dx in range(NX) for dy in range(NY) if dx or dy), key=lambda m: -far(m[0]) - far(m[1]))
    whole = [(dx, dy, dc) for dx, dy in moves for dc in (1, 0)] + [(0, 0, 1)]
    near = [sign * d for d in range(STRIDE, 0, -1) for sign in (1, -1)]

    barrier = pltpu.get_barrier_semaphore()
    for off in near:
        pl.semaphore_signal(barrier, inc=1, device_id=z_peer(off), device_id_type=MESH)
    for dx, dy in moves:
        pl.semaphore_signal(barrier, inc=1, device_id=plane_peer(dx, dy, 0)[0], device_id_type=MESH)
    pl.semaphore_signal(barrier, inc=1, device_id=plane_peer(0, 0, 1)[0], device_id_type=MESH)
    for cp in loads:
        cp.wait()
    pl.semaphore_wait(barrier, len(near) + len(moves) + 1)

    def slot_of(off):
        return 2 * off - 1 if off > 0 else -2 * off

    def send(src, dst, send_sem, recv_sem, peer):
        pltpu.make_async_remote_copy(
            src_ref=src, dst_ref=dst, send_sem=send_sem, recv_sem=recv_sem, device_id=peer, device_id_type=MESH).start()

    def send_z(source, step):
        to = slot_of(source + step)
        send(zbuf.at[slot_of(source) if source else 0], zbuf.at[to], zsend_sem, zrecv_sem.at[to], z_peer(step))

    for off in near:
        send_z(0, off)
    for dx, dy in moves:
        peer, _ = plane_peer(dx, dy, 0)
        send(zbuf.at[0], pbuf.at[q], psend_sem, precv_sem, peer)

    def wait_bytes(ref, sem):
        pltpu.make_async_copy(ref, ref, sem).wait()

    for hub in range(STRIDE, NZ // 2, STRIDE):
        for sign in (1, -1):
            at = slot_of(sign * hub)
            wait_bytes(zbuf.at[at], zrecv_sem.at[at])
            for step in range(min(STRIDE, NZ // 2 - hub - (sign < 0)), 0, -1):
                send_z(sign * hub, sign * step)
    hubs = [slot_of(sign * hub) for hub in range(STRIDE, NZ // 2, STRIDE) for sign in (1, -1)]

    wait_bytes(pbuf.at[pl.ds(0, NX * NY - 1)], precv_sem)
    half = pbuf.at[pl.ds(c * (NX * NY), NX * NY)]
    send(half, half, dsend_sem, drecv_sem, plane_peer(0, 0, 1)[0])

    acc[...] = jnp.zeros_like(acc)
    ones8 = jnp.ones((8, DIM), BF16)

    wait_bytes(half, drecv_sem)
    for g in range(TILES):
        for k in range(2):
            pts = pbuf[4 * g:4 * g + 4, PTS * k:PTS * k + PTS, :].reshape(128, DIM)
            high, low = squares(pts)
            norm = lax.dot_general(ones8, high, NT, preferred_element_type=F32)
            norm += lax.dot_general(ones8, low, NT, preferred_element_type=F32)
            rown[g, k] = norm * -SCALE

    def chunk(n, carry):
        for j in range(4):
            at = 4 * n + j
            ready = at == 0
            for hub in hubs:
                ready |= at == hub

            @pl.when(jnp.logical_not(ready))
            def _():
                wait_bytes(zbuf.at[at], zrecv_sem.at[at])

        cols = []
        for k in range(2):
            pts = zbuf[pl.ds(4 * n, 4), PTS * k:PTS * k + PTS, :].reshape(128, DIM)
            high, low = squares(pts)
            ones = jnp.ones((DIM, 128), BF16)
            norm = jnp.dot(high, ones, preferred_element_type=F32) + jnp.dot(low, ones, preferred_element_type=F32)
            coln[k] = norm * -SCALE
            cols.append(pts)
        cols = jnp.concatenate(cols, axis=0)
        own = jnp.where(n == 0, q * PTS, -PLANE * PTS)
        lane = lax.broadcasted_iota(jnp.int32, (PTS, 128), 1)
        sub = lax.broadcasted_iota(jnp.int32, (PTS, 128), 0) + own
        for g in range(TILES):
            rows_x = pbuf[4 * g:4 * g + 4, 0:PTS, :].reshape(128, DIM)
            rows_y = pbuf[4 * g:4 * g + 4, PTS:2 * PTS, :].reshape(128, DIM)
            prod_x = lax.dot_general(cols, rows_x, NT, preferred_element_type=F32)
            prod_y = lax.dot_general(cols, rows_y, NT, preferred_element_type=F32)
            part = [acc[g, i] for i in range(15)]
            for j in range(4):
                def gauss(prod, k, row):
                    arg = prod[128 * k + PTS * j:128 * k + PTS * j + PTS] * (2.0 * SCALE) + coln[k, PTS * j:PTS * j + PTS]
                    arg = (arg.reshape(-1, 8, 128) + rown[g, row][None]).reshape(PTS, 128)
                    return powers(jnp.exp2(jnp.minimum(arg, 0.0)))

                xx = gauss(prod_x, 0, 0)
                xy = gauss(prod_x, 1, 0)
                yx = gauss(prod_y, 0, 1)
                yy = gauss(prod_y, 1, 1)
                hh = [a * b for a, b in zip(xx, yy)]
                if j == 0:
                    off = lane + 128 * g != sub
                    xx = [jnp.where(off, a, 0.0) for a in xx]
                    yy = [jnp.where(off, a, 0.0) for a in yy]
                for t, stat in enumerate((xx, yy, xy, yx, hh)):
                    for b in range(3):
                        part[t * 3 + b] += fold(stat[b])
            for i in range(15):
                acc[g, i] = part[i]
        return carry

    lax.fori_loop(0, NZ // 4, chunk, 0)

    for g in range(TILES):
        def row(t, b):
            return jnp.sum(acc[g, t * 3 + b], axis=0, keepdims=True)
        zero = jnp.zeros((1, 128), F32)
        groups = [jnp.concatenate([row(k, 0), row(k, 1), row(k, 2), row(4, k) if k < 3 else zero], axis=0) for k in range(4)]
        for m in range(4):
            sbuf[4 * g + m] = jnp.concatenate([groups[k][:, PTS * m:PTS * m + PTS] for k in range(4)], axis=1)

    for move in whole:
        peer, to = plane_peer(*move)
        send(sbuf.at[to], rbuf.at[q], ssend_sem, srecv_sem, peer)
    rbuf[q] = sbuf[q]
    wait_bytes(rbuf.at[pl.ds(0, PLANE - 1)], srecv_sem)
    sums = jnp.sum(rbuf[...], axis=0)
    full = sums + 1.0
    prod = full * pltpu.roll(full, 128 - PTS, 1)
    lane = lax.broadcasted_iota(jnp.int32, (4, 128), 1)
    sub = lax.broadcasted_iota(jnp.int32, (4, 128), 0)
    packed = jnp.zeros((4, 128), F32)
    for k in range(5):
        src = prod if k == 4 else sums
        lo = PTS * (k % 4)
        tot = jnp.sum(jnp.where((lane >= lo) & (lane < lo + PTS), src, 0.0), axis=1, keepdims=True)
        packed = jnp.where(lane == 8 * sub + k, tot, packed)
    tsend[...] = jnp.sum(packed, axis=0, keepdims=True)

    for move in whole:
        send(tsend, trecv.at[q], tsend_sem, trecv_sem, plane_peer(*move)[0])
    trecv[q] = tsend[...]

    logs = jnp.log(sums)
    score = logs - pltpu.roll(logs, 64, 1)
    xs_ref[...] = score[0:3, 0:PTS]
    ys_ref[...] = score[0:3, PTS:2 * PTS]

    wait_bytes(trecv.at[pl.ds(0, PLANE - 1)], trecv_sem)
    usend[...] = jnp.sum(trecv[...], axis=0)
    for off in [NZ // 2] + [sign * d for d in range(NZ // 2 - 1, 0, -1) for sign in (1, -1)]:
        send(usend, urecv.at[z], usend_sem, urecv_sem, z_peer(off))
    urecv[z] = usend[...]
    wait_bytes(urecv.at[pl.ds(0, NZ - 1)], urecv_sem)
    tot = jnp.sum(urecv[...], axis=0)

    n = float(PTS * PLANE * NZ)

    def at(k, b):
        return tot[0:1, 8 * b + k:8 * b + k + 1]

    for b in range(3):
        txx, tyy, txy, tpr = at(0, b), at(1, b), at(2, b), at(4, b)
        th = tot[0:1, 8 * 3 + b:8 * 3 + b + 1]
        mmd_ref[0:1, b:b + 1] = n * ((txx + tyy) / (n * (n - 1.0)) - 2.0 * txy / (n * n))
        hsic_ref[0:1, b:b + 1] = (th - 2.0 * tpr / n + (txx + n) * (tyy + n) / (n * n)) / n

    wait_bytes(zbuf.at[pl.ds(0, NZ - 1)], zsend_sem)
    wait_bytes(pbuf.at[pl.ds(0, NX * NY - 1)], psend_sem)
    wait_bytes(half, dsend_sem)
    wait_bytes(sbuf.at[pl.ds(0, PLANE - 1)], ssend_sem)
    wait_bytes(trecv.at[pl.ds(0, PLANE - 1)], tsend_sem)
    wait_bytes(urecv.at[pl.ds(0, NZ - 1)], usend_sem)


def shards(x_points, y_points):
    dma = pltpu.SemaphoreType.DMA
    vmem = pl.BlockSpec(memory_space=pltpu.VMEM)
    xs, ys, mmd, hsic = pl.pallas_call(
        kernel,
        out_shape=(
            jax.ShapeDtypeStruct((3, PTS), F32),
            jax.ShapeDtypeStruct((3, PTS), F32),
            jax.ShapeDtypeStruct((1, 3), F32),
            jax.ShapeDtypeStruct((1, 3), F32),
        ),
        in_specs=[pl.BlockSpec(memory_space=pl.ANY)] * 2,
        out_specs=(vmem,) * 4,
        scratch_shapes=[
            pltpu.VMEM((NZ, 2 * PTS, DIM), BF16),
            pltpu.VMEM((PLANE, 2 * PTS, DIM), BF16),
            pltpu.VMEM((TILES, 2, 8, 128), F32),
            pltpu.VMEM((2, 128, 128), F32),
            pltpu.VMEM((TILES, 15, 8, 128), F32),
            pltpu.VMEM((PLANE, 4, 128), F32),
            pltpu.VMEM((PLANE, 4, 128), F32),
            pltpu.VMEM((1, 128), F32),
            pltpu.VMEM((PLANE, 1, 128), F32),
            pltpu.VMEM((1, 128), F32),
            pltpu.VMEM((NZ, 1, 128), F32),
            dma((4,)), dma, dma((NZ,)), dma, dma, dma, dma, dma, dma, dma, dma, dma, dma,
        ],
        compiler_params=pltpu.CompilerParams(collective_id=0, has_side_effects=True),
        name="mmd_hsic",
    )(x_points, y_points)
    return xs.T, ys.T, mmd.reshape(3), hsic.reshape(3)


def solution(mesh):
    return jax.shard_map(
        shards,
        mesh=mesh,
        in_specs=(P("blk", None), P("blk", None)),
        out_specs=(P("blk", None), P("blk", None), P(), P()),
        check_vma=False,
    )
```
